128 devices in a mesh: ax: 8 (over x, core), rad: 16 (over z, y).
Axes of the slice: x: 4, y: 4, z: 4, core: 2. Of those that a mesh axis runs over, the one named last changes fastest.
Arguments:
- sources: float32 [16, 32, 200, 128], P('ax', 'rad'), may hold values from -0.6 to 0.6
- block_inverse: float32 [16, 32, 200, 200], P('ax', 'rad'), may hold values from -2 to 2, as said below
- radial_coupling: float32 [16, 32, 2, 200], P('ax', 'rad'), may hold values from 0.2 to 1.2
- axial_coupling: float32 [16, 32, 4, 200], P('ax', 'rad'), may hold values from 0.01 to 0.05
Outputs:
- correction: float32 [16, 32, 200, 128], P('ax', 'rad')
The draws below stay inside these ranges and needn't reach their ends.
Inputs may be any that keep to these rules, and one draw needn't show every extreme that they name: `block_inverse`: the given inverse of each cell's diagonal block.
All inputs are finite; a program needn't handle non-finite values.
Results may differ from the reference program's by a relative error of at most 0.00014.
Values sent between devices are 32-bit elements; how exact they have to be, the bound alone decides.
No kernel may reach another device: no remote copies, remote signals or barrier semaphores. Data moves between devices by JAX's collectives and lax.ppermute only.
A program may use at most 64 MiB of HBM per device.

```python
import math
import jax
import jax.numpy as jnp
from jax import lax

S = 200
K = 128
SWEEPS = 2
NA = 16
NR = 32


def draw_block_inverse(key, part):
    key_diag, key_off = jax.random.split(jax.random.fold_in(key, 11), 2)
    diagonal = jax.random.uniform(key_diag, (NA, NR, S), jnp.float32, 0.8, 1.2)
    spread = jax.random.normal(key_off, (NA, NR, S, S), jnp.float32) * (0.25 / math.sqrt(S))
    spread = jnp.clip(spread, -0.5, 0.5)
    return spread + diagonal[..., None] * jnp.eye(S, dtype=jnp.float32)


def draw_radial_coupling(key, part):
    key_rate, key_rough = jax.random.split(jax.random.fold_in(key, 23), 2)
    species_rate = jax.random.uniform(key_rate, (2, S), jnp.float32, 0.35, 0.9)
    roughness = jax.random.uniform(key_rough, (NA, NR, 2, S), jnp.float32, 0.65, 1.3)
    return species_rate * roughness


def block_levels(stream_key, extent, cuts, least, high):
    loudness = 1.0
    for dim, parts in cuts:
        heights = jax.random.uniform(jax.random.fold_in(jax.random.fold_in(stream_key, 6), dim), (parts,), jnp.float32, least / len(cuts), high / len(cuts))
        loudness = loudness * jnp.repeat(jnp.exp(heights), extent[dim] // parts).reshape((-1,) + (1,) * (len(extent) - 1 - dim))
    return loudness


def normal_values(own_key, dims, width, bound, shards=(), kind=jnp.bfloat16):
    values = jax.random.normal(own_key, dims, jnp.float32) * width
    if len(shards) > 0:
        values = block_levels(own_key, dims, shards, -0.22, 0.18) * values
    return jnp.clip(values, min=-bound, max=bound).astype(kind)


def setup_inputs(seed: int = 0) -> dict:
    streams_of = jax.random.split(jax.random.key(seed), 5)
    sources = normal_values(streams_of[0], (NA, NR, S, K), 0.1, 0.6, ((0, 8), (1, 16)), jnp.float32)
    block_inverse = draw_block_inverse(jax.random.fold_in(streams_of[4], 71), 0)
    radial_coupling = draw_radial_coupling(jax.random.fold_in(streams_of[4], 71), 0)
    axial_coupling = jnp.clip(0.01 + 0.04 * jax.random.uniform(streams_of[3], (NA, NR, 4, S), jnp.float32) ** block_levels(streams_of[3], (NA, NR, 4, S), ((0, 8), (1, 16)), -0.2, 0.2), 0.01, 0.05)
    return {"sources": sources, "block_inverse": block_inverse, "radial_coupling": radial_coupling, "axial_coupling": axial_coupling}


def forward_line(line_source, block_inverse, inward_coupling):
    def advance(previous, entries):
        source_row, inverse_row, coupling_row = entries
        shifted = source_row - coupling_row[..., None] * previous
        current = jnp.einsum('aij,ajk->aik', inverse_row, shifted, precision=lax.Precision.HIGHEST)
        return current, current
    initial = jnp.zeros((NA, S, K), jnp.float32)
    _, values = lax.scan(advance, initial, (jnp.moveaxis(line_source, 1, 0), jnp.moveaxis(block_inverse, 1, 0), jnp.moveaxis(inward_coupling, 1, 0)))
    return jnp.moveaxis(values, 0, 1)


def backward_line(inner_value, block_inverse, outward_coupling):
    def retreat(following, entries):
        inner_row, inverse_row, coupling_row = entries
        shifted = coupling_row[..., None] * following
        current = inner_row - jnp.einsum('aij,ajk->aik', inverse_row, shifted, precision=lax.Precision.HIGHEST)
        return current, current
    initial = jnp.zeros((NA, S, K), jnp.float32)
    _, values = lax.scan(retreat, initial, (jnp.moveaxis(inner_value, 1, 0), jnp.moveaxis(block_inverse, 1, 0), jnp.moveaxis(outward_coupling, 1, 0)), reverse=True)
    return jnp.moveaxis(values, 0, 1)


def reference(sources, block_inverse, radial_coupling, axial_coupling):
    correction = jnp.zeros((NA, NR, S, K), jnp.float32)
    for sweep_index in range(SWEEPS):
        if sweep_index == 0:
            line_source = sources
        else:
            padded = jnp.pad(correction, ((2, 2), (0, 0), (0, 0), (0, 0)))
            line_source = sources
            line_source = line_source - axial_coupling[:, :, 0, :, None] * padded[0:NA]
            line_source = line_source - axial_coupling[:, :, 1, :, None] * padded[1:NA + 1]
            line_source = line_source - axial_coupling[:, :, 2, :, None] * padded[3:NA + 3]
            line_source = line_source - axial_coupling[:, :, 3, :, None] * padded[4:NA + 4]
        inner_value = forward_line(line_source, block_inverse, radial_coupling[:, :, 0])
        correction = backward_line(inner_value, block_inverse, radial_coupling[:, :, 1])
    return correction
```

```python
import jax
import jax.numpy as jnp
from jax import lax
from jax.experimental import pallas as pl
from jax.experimental.pallas import tpu as pltpu
from jax.sharding import Mesh
from jax.sharding import PartitionSpec as P

SWEEPS = 2
RAD = ("rad_0", "rad_1")
GROUP = 4
F32 = jnp.float32
BF16 = jnp.bfloat16


def split(value):
    high = value.astype(BF16)
    return high, (value - high.astype(F32)).astype(BF16)


def dot(a, b, contract):
    dims = (((1,), (contract,)), ((), ()))
    return lax.dot_general(a, b, dims, preferred_element_type=F32)


def times(value, high, low, contract):
    value_high, value_low = split(value)
    return (
        dot(value_high, high, contract)
        + dot(value_low, high, contract)
        + dot(value_high, low, contract)
    )


def call(body, out, flops, scratch=(), scalars=0):
    def run(*operands):
        specs = [pl.BlockSpec(memory_space=pltpu.SMEM)] * scalars
        specs += [pl.BlockSpec(memory_space=pltpu.VMEM)] * (len(operands) - scalars)
        moved = sum(o.size * o.dtype.itemsize for o in operands)
        return pl.pallas_call(
            body,
            out_shape=[jax.ShapeDtypeStruct(shape, kind) for shape, kind in out],
            in_specs=specs,
            out_specs=[pl.BlockSpec(memory_space=pltpu.VMEM)] * len(out),
            scratch_shapes=list(scratch),
            name=body.__name__,
            cost_estimate=pl.CostEstimate(
                flops=flops, transcendentals=0, bytes_accessed=moved
            ),
            compiler_params=pltpu.CompilerParams(vmem_limit_bytes=48 * 1024 * 1024),
        )(*operands)

    return run


def pack(mine_ref, sources_ref, radial_ref, axial_ref, m0, m1, m2, m3, turned):
    mine = mine_ref[0]
    width = m0.shape[2] - 8
    for station in range(sources_ref.shape[0]):
        for cell in range(sources_ref.shape[1]):
            turned[...] = sources_ref[station, cell].T
            for ahead, message in enumerate((m0, m1, m2, m3)):
                row = pl.multiple_of(lax.rem(mine + ahead, GROUP) * width, 8)
                message[station, cell, 0:width] = turned[pl.ds(row, width)]
                message[station, cell, width : width + 2] = radial_ref[station, cell]
                message[station, cell, width + 2 : width + 6] = axial_ref[station, cell]
                message[station, cell, width + 6 : width + 8] = jnp.zeros(
                    (2, turned.shape[1]), F32
                )


def first_inner(
    mine_ref, b0, b1, b2a, b2b, b3, m0, m1, m2, m3,
    fields, high, low, local, carry_high, carry_low, last, chain,
):
    mine = mine_ref[0]
    cells = b0.shape[1]
    width = local.shape[2]
    species = b0.shape[2]
    for station in range(2):
        opposite = (b2a, b2b)[station]
        for ahead in range(GROUP):
            base = lax.rem(mine + ahead, GROUP) * cells
            for cell in range(cells):
                if ahead == 2:
                    block = opposite[0, cell]
                else:
                    block = (b0, b1, None, b3)[ahead][station, cell]
                block_high, block_low = split(block)
                high[station, base + cell] = block_high
                low[station, base + cell] = block_low
                fields[station, base + cell] = (m0, m1, m2, m3)[ahead][station, cell]
    rows = lax.broadcasted_iota(jnp.int32, (species, species), 0)
    lanes = lax.broadcasted_iota(jnp.int32, (species, species), 1)
    unit = jnp.where(rows == lanes, 1.0, 0.0).astype(F32)
    matrix = [unit, unit]
    value = [None, None]
    for cell in range(GROUP * cells):
        for station in range(2):
            coupling = fields[station, cell, width : width + 1]
            shifted = fields[station, cell, 0:width]
            if cell:
                shifted = shifted - coupling * value[station]
            block_high, block_low = high[station, cell], low[station, cell]
            value[station] = times(shifted, block_high, block_low, 1)
            matrix[station] = times(-coupling * matrix[station], block_high, block_low, 1)
            local[station, cell] = value[station]
            part_high, part_low = split(matrix[station])
            carry_high[station, cell] = part_high
            carry_low[station, cell] = part_low
    for station in range(2):
        last[station] = value[station]
        chain[station] = matrix[station]


def outer_matrices(fields, high, low, carry_high, carry_low, chain):
    cells = high.shape[1]
    species = high.shape[2]
    width = fields.shape[2] - 8
    rows = lax.broadcasted_iota(jnp.int32, (species, species), 0)
    lanes = lax.broadcasted_iota(jnp.int32, (species, species), 1)
    unit = jnp.where(rows == lanes, 1.0, 0.0).astype(F32)
    matrix = [unit, unit]
    for cell in reversed(range(cells)):
        for station in range(2):
            coupling = fields[station, cell, width + 1 : width + 2]
            matrix[station] = times(
                -coupling * matrix[station], high[station, cell], low[station, cell], 1
            )
            part_high, part_low = split(matrix[station])
            carry_high[station, cell] = part_high
            carry_low[station, cell] = part_low
    for station in range(2):
        chain[station] = matrix[station]


def advance(ends, near, carry_high, carry_low, cell, joined):
    for station in range(2):
        joined[station] = ends[station] + times(
            near[station], carry_high[station, cell], carry_low[station, cell], 0
        )


def advance_inner(ends, near, carry_high, carry_low, joined):
    advance(ends, near, carry_high, carry_low, carry_high.shape[1] - 1, joined)


def advance_outer(ends, near, carry_high, carry_low, joined):
    advance(ends, near, carry_high, carry_low, 0, joined)


def incoming(near, middle, far, chain, station):
    matrix_high, matrix_low = split(chain[station])
    return near[station] + middle[station] + times(far[station], matrix_high, matrix_low, 0)


def outer_local(
    near, middle, far, chain, inner, carry_high, carry_low, fields, high, low, local, last
):
    cells = inner.shape[1]
    width = inner.shape[2]
    arriving = [incoming(near, middle, far, chain, station) for station in range(2)]
    value = [None, None]
    for cell in reversed(range(cells)):
        for station in range(2):
            whole = inner[station, cell] + times(
                arriving[station], carry_high[station, cell], carry_low[station, cell], 0
            )
            if value[station] is not None:
                coupling = fields[station, cell, width + 1 : width + 2]
                whole = whole - times(
                    coupling * value[station], high[station, cell], low[station, cell], 1
                )
            value[station] = whole
            local[station, cell] = whole
    for station in range(2):
        last[station] = value[station]


def finish(near, middle, far, chain, outer, carry_high, carry_low, correction):
    for station in range(2):
        arriving = incoming(near, middle, far, chain, station)
        for cell in range(outer.shape[1]):
            correction[station, cell] = outer[station, cell] + times(
                arriving, carry_high[station, cell], carry_low[station, cell], 0
            )


def next_inner(below, own, above, fields, high, low, local, last):
    cells = own.shape[1]
    width = own.shape[2]
    value = [None, None]
    for cell in range(cells):
        around = [part[s, cell] for part in (below, own, above) for s in range(2)]
        for station in range(2):
            source = fields[station, cell, 0:width]
            for term, place in enumerate((0, 1, 3, 4)):
                factor = fields[station, cell, width + 2 + term : width + 3 + term]
                source = source - factor * around[station + place]
            if value[station] is not None:
                coupling = fields[station, cell, width : width + 1]
                source = source - coupling * value[station]
            value[station] = times(source, high[station, cell], low[station, cell], 1)
            local[station, cell] = value[station]
    for station in range(2):
        last[station] = value[station]


def finish_last(
    mine_ref, near, middle, far, chain, outer, carry_high, carry_low, m0, m1, m2, m3, whole
):
    finish(near, middle, far, chain, outer, carry_high, carry_low, whole)
    mine = mine_ref[0]
    cells = m0.shape[1]
    for station in range(2):
        for ahead, message in enumerate((m0, m1, m2, m3)):
            base = lax.rem(mine + ahead, GROUP) * cells
            for cell in range(cells):
                message[station, cell] = whole[station, base + cell]


def unpack(mine_ref, m0, m1, m2, m3, correction, turned):
    mine = mine_ref[0]
    width = m0.shape[2]
    for station in range(2):
        for cell in range(m0.shape[1]):
            for ahead, message in enumerate((m0, m1, m2, m3)):
                row = pl.multiple_of(lax.rem(mine + ahead, GROUP) * width, 8)
                turned[pl.ds(row, width)] = message[station, cell]
            correction[station, cell] = turned[...].T


def shift(value, axis, step):
    count = lax.axis_size(axis)
    return lax.ppermute(value, axis, [(i, (i + step) % count) for i in range(count)])


def scan(ends, carry, chain, step, pairs, then, advance_body):
    stations, width, species = ends.shape
    near = lax.ppermute(ends, "rad_0", pairs)
    (joined,) = call(advance_body, [(ends.shape, F32)], 6 * stations * width * species**2)(
        ends, near, *carry
    )
    middle = lax.ppermute(joined, "rad_0", [then[0]])
    far = lax.ppermute(joined, "rad_0", [then[1]])
    return near, middle, far, chain


def on_device(sources, block_inverse, radial_coupling, axial_coupling):
    stations, own_cells, species, columns = sources.shape
    cells = own_cells * GROUP
    width = columns // GROUP
    mine = lax.axis_index("rad_1").astype(jnp.int32).reshape(1)
    step = 6 * stations * cells * species**2
    field = (stations, cells, width, species)
    square = (stations, cells, species, species)
    edge = (stations, width, species)

    half = [block_inverse[s : s + 1] for s in range(2)]
    below = [None, None]
    above = [None, None]
    below[0] = shift(half[0], "rad_1", 1)
    above[1] = shift(half[1], "rad_1", -1)
    message = [(stations, own_cells, width + 8, species)] * GROUP
    sent = call(
        pack,
        [(shape, F32) for shape in message],
        1000,
        scratch=[pltpu.VMEM((columns, species), F32)],
        scalars=1,
    )(mine, sources, radial_coupling, axial_coupling)
    got = [sent[0]] + [None] * 3
    for ahead in range(1, GROUP):
        got[GROUP - ahead] = shift(sent[ahead], "rad_1", ahead)
    below[1] = shift(half[1], "rad_1", 1)
    above[0] = shift(half[0], "rad_1", -1)
    across = [shift(below[0], "rad_1", 1), shift(above[1], "rad_1", -1)]
    below_all = jnp.concatenate(below, 0)
    above_all = jnp.concatenate(above, 0)

    fields, high, low, inner, in_high, in_low, last, in_chain = call(
        first_inner,
        [
            ((stations, cells, width + 8, species), F32),
            (square, BF16),
            (square, BF16),
            (field, F32),
            (square, BF16),
            (square, BF16),
            (edge, F32),
            ((stations, species, species), F32),
        ],
        step * (width + species),
        scalars=1,
    )(mine, block_inverse, above_all, *across, below_all, *got)
    in_next = lax.ppermute(in_chain, "rad_0", [(2, 3)])
    inner_carry = (in_high, in_low)
    arriving = scan(last, inner_carry, in_next, step, [(0, 1), (2, 3)], [(1, 2), (1, 3)], advance_inner)
    out_high, out_low, out_chain = call(
        outer_matrices,
        [(square, BF16), (square, BF16), ((stations, species, species), F32)],
        step * species,
    )(fields, high, low)
    out_next = lax.ppermute(out_chain, "rad_0", [(1, 0)])
    outer_carry = (out_high, out_low)

    for sweep_index in range(SWEEPS):
        if sweep_index:
            count = lax.axis_size("ax")
            up = lax.ppermute(correction, "ax", [(i, i + 1) for i in range(count - 1)])
            down = lax.ppermute(correction, "ax", [(i + 1, i) for i in range(count - 1)])
            inner, last = call(next_inner, [(field, F32), (edge, F32)], step * width)(
                up, correction, down, fields, high, low
            )
            arriving = scan(
                last, inner_carry, in_next, step, [(0, 1), (2, 3)], [(1, 2), (1, 3)], advance_inner
            )
        outer, last = call(outer_local, [(field, F32), (edge, F32)], 2 * step * width)(
            *arriving, inner, *inner_carry, fields, high, low
        )
        arriving = scan(
            last, outer_carry, out_next, step, [(1, 0), (3, 2)], [(2, 1), (2, 0)], advance_outer
        )
        if sweep_index + 1 < SWEEPS:
            (correction,) = call(finish, [(field, F32)], step * width)(
                *arriving, outer, *outer_carry
            )
    message = [(stations, own_cells, width, species)] * GROUP
    sent = call(
        finish_last,
        [(shape, F32) for shape in message],
        step * width,
        scratch=[pltpu.VMEM(field, F32)],
        scalars=1,
    )(mine, *arriving, outer, *outer_carry)
    got = [sent[0]] + [None] * 3
    for ahead in range(1, GROUP):
        got[GROUP - ahead] = shift(sent[ahead], "rad_1", ahead)
    (correction,) = call(
        unpack,
        [(sources.shape, F32)],
        1000,
        scratch=[pltpu.VMEM((columns, species), F32)],
        scalars=1,
    )(mine, *got)
    return correction


def solution(mesh):
    torus = Mesh(mesh.devices.reshape(mesh.shape["ax"], GROUP, GROUP), ("ax", "rad_0", "rad_1"))
    placed = (P("ax", RAD, None, None),) * 4
    return jax.shard_map(
        on_device, mesh=torus, in_specs=placed, out_specs=P("ax", RAD, None, None), check_vma=False
    )
```

```python
import jax
import jax.numpy as jnp
from jax import lax
from jax.experimental import pallas as pl
from jax.experimental.pallas import tpu as pltpu
from jax.sharding import Mesh
from jax.sharding import PartitionSpec as P

SWEEPS = 2
RAD = ("rad_0", "rad_1")
GROUP = 4
F32 = jnp.float32
BF16 = jnp.bfloat16


def split(value):
    high = value.astype(BF16)
    return high, (value - high.astype(F32)).astype(BF16)


def dot(a, b, contract):
    dims = (((1,), (contract,)), ((), ()))
    return lax.dot_general(a, b, dims, preferred_element_type=F32)


def times(value, high, low, contract):
    value_high, value_low = split(value)
    return (
        dot(value_high, high, contract)
        + dot(value_low, high, contract)
        + dot(value_high, low, contract)
    )


def call(body, out, scratch=(), scalars=0):
    def run(*operands):
        specs = [pl.BlockSpec(memory_space=pltpu.SMEM)] * scalars
        specs += [pl.BlockSpec(memory_space=pltpu.VMEM)] * (len(operands) - scalars)
        return pl.pallas_call(
            body,
            out_shape=[jax.ShapeDtypeStruct(shape, kind) for shape, kind in out],
            in_specs=specs,
            out_specs=[pl.BlockSpec(memory_space=pltpu.VMEM)] * len(out),
            scratch_shapes=list(scratch),
            cost_estimate=pl.CostEstimate(
                flops=1000, transcendentals=0, bytes_accessed=1000
            ),
            compiler_params=pltpu.CompilerParams(vmem_limit_bytes=12 * 1024 * 1024),
        )(*operands)

    return run


def pack_blocks(block_ref, radial_ref, axial_ref, first, second):
    for station, packed in enumerate((first, second)):
        for cell in range(2):
            packed[200 * cell : 200 * cell + 200] = block_ref[station, cell, :, 0:128]
            packed[400:600, 64 * cell : 64 * cell + 64] = block_ref[station, cell, :, 128:192]
            for chunk in range(7):
                start, stop = 32 * chunk, min(32 * chunk + 32, 200)
                lane = 16 * chunk + 8 * cell
                packed[600 : 600 + stop - start, lane : lane + 8] = block_ref[
                    station, cell, start:stop, 192:200
                ]
            low = 632 + 8 * cell
            packed[low : low + 2] = radial_ref[station, cell, :, 0:128]
            packed[low + 2 : low + 6] = axial_ref[station, cell, :, 0:128]
            packed[low + 16 : low + 18, 0:72] = radial_ref[station, cell, :, 128:200]
            packed[low + 18 : low + 22, 0:72] = axial_ref[station, cell, :, 128:200]


def unpack_block(packed, cell, whole, coupling_whole):
    whole[:, 0:128] = packed[200 * cell : 200 * cell + 200]
    whole[:, 128:192] = packed[400:600, 64 * cell : 64 * cell + 64]
    for chunk in range(7):
        start, stop = 32 * chunk, min(32 * chunk + 32, 200)
        lane = 16 * chunk + 8 * cell
        whole[start:stop, 192:200] = packed[600 : 600 + stop - start, lane : lane + 8]
    low = 632 + 8 * cell
    coupling_whole[:, 0:128] = packed[low : low + 8]
    coupling_whole[:, 128:200] = packed[low + 16 : low + 24, 0:72]
    return split(whole[...]) + (coupling_whole[...],)


def take_near(own0, own1, above0, above1, below0, below1, high, low, coupling, whole, rows):
    for place, pair in enumerate(((own0, own1), (above0, above1), (below0, below1))):
        for station in range(2):
            for cell in range(2):
                block_high, block_low, couple = unpack_block(pair[station], cell, whole, rows)
                high[place, station, cell] = block_high
                low[place, station, cell] = block_low
                coupling[place, station, cell] = couple


def unit_matrix(species):
    rows = lax.broadcasted_iota(jnp.int32, (species, species), 0)
    lanes = lax.broadcasted_iota(jnp.int32, (species, species), 1)
    return jnp.where(rows == lanes, 1.0, 0.0).astype(F32)


def inner_matrices(
    mine_ref, near_high, near_low, near_coupling, across0, across1,
    high, low, coupling, carry, chain, whole, rows,
):
    mine = mine_ref[0]
    for ahead, place in ((0, 0), (1, 1), (3, 2), (2, None)):
        base = lax.rem(mine + ahead, GROUP) * 2
        for station in range(2):
            for cell in range(2):
                if place is None:
                    packed = (across0, across1)[station]
                    parts = unpack_block(packed, cell, whole, rows)
                else:
                    parts = tuple(
                        near[place, station, cell]
                        for near in (near_high, near_low, near_coupling)
                    )
                high[station, base + cell] = parts[0]
                low[station, base + cell] = parts[1]
                coupling[station, base + cell] = parts[2]
    matrix = [unit_matrix(high.shape[2])] * 2
    for cell in range(high.shape[1]):
        for station in range(2):
            inward = coupling[station, cell, 0:1]
            matrix[station] = times(
                -inward * matrix[station], high[station, cell], low[station, cell], 1
            )
            carry[station, cell] = matrix[station]
    for station in range(2):
        chain[station] = matrix[station]


def outer_matrices(high, low, coupling, carry_high, carry_low, chain):
    matrix = [unit_matrix(high.shape[2])] * 2
    for cell in reversed(range(high.shape[1])):
        for station in range(2):
            outward = coupling[station, cell, 1:2]
            matrix[station] = times(
                -outward * matrix[station], high[station, cell], low[station, cell], 1
            )
            part_high, part_low = split(matrix[station])
            carry_high[station, cell] = part_high
            carry_low[station, cell] = part_low
    for station in range(2):
        chain[station] = matrix[station]


def turned_matrices(high, low, coupling, carry, turn_high, turn_low, first):
    matrix = [None, None]
    for cell in reversed(range(high.shape[1])):
        for station in range(2):
            whole = carry[station, cell]
            if matrix[station] is not None:
                outward = coupling[station, cell, 1:2]
                whole = whole - times(
                    outward * matrix[station], high[station, cell], low[station, cell], 1
                )
            matrix[station] = whole
            part_high, part_low = split(whole)
            turn_high[station, cell] = part_high
            turn_low[station, cell] = part_low
    for station in range(2):
        first[station] = matrix[station]


def pack(mine_ref, sources_ref, m0, m1, m2, m3, turned):
    mine = mine_ref[0]
    width = m0.shape[2]
    for station in range(2):
        for cell in range(2):
            turned[...] = sources_ref[station, cell].T
            for ahead, message in enumerate((m0, m1, m2, m3)):
                row = pl.multiple_of(lax.rem(mine + ahead, GROUP) * width, 8)
                message[station, cell] = turned[pl.ds(row, width)]


def first_inner(mine_ref, m0, m1, m2, m3, high, low, coupling, sources, local, last):
    mine = mine_ref[0]
    for station in range(2):
        for ahead, message in enumerate((m0, m1, m2, m3)):
            base = lax.rem(mine + ahead, GROUP) * 2
            for cell in range(2):
                sources[station, base + cell] = message[station, cell]
    inner_chain(lambda station, cell: sources[station, cell], high, low, coupling, local, last)


def inner_chain(source_of, high, low, coupling, local, last):
    value = [None, None]
    for cell in range(high.shape[1]):
        for station in range(2):
            shifted = source_of(station, cell)
            if value[station] is not None:
                shifted = shifted - coupling[station, cell, 0:1] * value[station]
            value[station] = times(shifted, high[station, cell], low[station, cell], 1)
            local[station, cell] = value[station]
    for station in range(2):
        last[station] = value[station]


def next_inner(below, own, above, sources, high, low, coupling, local, last):
    def source_of(station, cell):
        around = [part[s, cell] for part in (below, own, above) for s in range(2)]
        source = sources[station, cell]
        for term, place in enumerate((0, 1, 3, 4)):
            source = source - coupling[station, cell, 2 + term : 3 + term] * around[station + place]
        return source

    inner_chain(source_of, high, low, coupling, local, last)


def outer_local(inner, high, low, coupling, local, last):
    value = [None, None]
    for cell in reversed(range(high.shape[1])):
        for station in range(2):
            whole = inner[station, cell]
            if value[station] is not None:
                shifted = coupling[station, cell, 1:2] * value[station]
                whole = whole - times(shifted, high[station, cell], low[station, cell], 1)
            value[station] = whole
            local[station, cell] = whole
    for station in range(2):
        last[station] = value[station]


def by_matrix(value, matrix):
    high, low = split(matrix)
    return times(value, high, low, 0)


def join_plain(ends, near, chain, joined):
    for station in range(2):
        joined[station] = ends[station] + by_matrix(near[station], chain[station])


def join(place_ref, ends, near, chain, chain_beside, joined):
    outermost = place_ref[0] == 0
    for station in range(2):
        mine, other = ends[station], near[station]
        matrix = jnp.where(outermost, chain_beside[station], chain[station])
        joined[station] = jnp.where(outermost, other, mine) + by_matrix(
            jnp.where(outermost, mine, other), matrix
        )


def incoming(place_ref, near, middle, chain_beside, station):
    place = place_ref[0]
    far = by_matrix(middle[station], chain_beside[station])
    arriving = near[station] + jnp.where(place == GROUP - 1, far, middle[station])
    return jnp.where(place == 0, 0.0, arriving)


def turn_first(near, middle, far, chain_beside, ends, matrix, arriving, turned):
    for station in range(2):
        value = near[station] + middle[station] + by_matrix(far[station], chain_beside[station])
        arriving[station] = value
        turned[station] = ends[station] + by_matrix(value, matrix[station])


def turn(place_ref, near, middle, chain_beside, ends, matrix, arriving, turned):
    for station in range(2):
        value = incoming(place_ref, near, middle, chain_beside, station)
        arriving[station] = value
        turned[station] = ends[station] + by_matrix(value, matrix[station])


def deepen(arriving, outer, turn_high, turn_low, deeper):
    for station in range(2):
        value = arriving[station]
        for cell in range(outer.shape[1]):
            deeper[station, cell] = outer[station, cell] + times(
                value, turn_high[station, cell], turn_low[station, cell], 0
            )


def finish(place_ref, near, middle, chain_beside, outer, carry_high, carry_low, correction):
    for station in range(2):
        arriving = incoming(place_ref, near, middle, chain_beside, station)
        for cell in range(outer.shape[1]):
            correction[station, cell] = outer[station, cell] + times(
                arriving, carry_high[station, cell], carry_low[station, cell], 0
            )


def finish_last(
    place_ref, mine_ref, near, middle, chain_beside, outer, carry_high, carry_low,
    m0, m1, m2, m3, whole,
):
    finish(place_ref, near, middle, chain_beside, outer, carry_high, carry_low, whole)
    mine = mine_ref[0]
    for station in range(2):
        for ahead, message in enumerate((m0, m1, m2, m3)):
            base = lax.rem(mine + ahead, GROUP) * 2
            for cell in range(2):
                message[station, cell] = whole[station, base + cell]


def unpack(mine_ref, m0, m1, m2, m3, correction, turned):
    mine = mine_ref[0]
    width = m0.shape[2]
    for station in range(2):
        for cell in range(2):
            for ahead, message in enumerate((m0, m1, m2, m3)):
                row = pl.multiple_of(lax.rem(mine + ahead, GROUP) * width, 8)
                turned[pl.ds(row, width)] = message[station, cell]
            correction[station, cell] = turned[...].T


def shift(value, axis, step):
    count = lax.axis_size(axis)
    return lax.ppermute(value, axis, [(i, (i + step) % count) for i in range(count)])


def hop(value, pairs):
    return lax.ppermute(value, "rad_0", pairs)


def mirrored(pairs):
    return [(GROUP - 1 - source, GROUP - 1 - target) for source, target in pairs]


def relax(sources, block_inverse, radial_coupling, axial_coupling):
    stations, own_cells, species, columns = sources.shape
    cells = own_cells * GROUP
    width = columns // GROUP
    mine = lax.axis_index("rad_1").astype(jnp.int32).reshape(1)
    place = lax.axis_index("rad_0").astype(jnp.int32).reshape(1)
    places = (place, GROUP - 1 - place)
    field = ((stations, cells, width, species), F32)
    square = ((stations, cells, species, species), BF16)
    wide = ((stations, cells, species, species), F32)
    edge = ((stations, width, species), F32)
    single = ((stations, species, species), F32)
    message = [((stations, own_cells, width, species), F32)] * GROUP
    rows = [pltpu.VMEM((species, species), F32), pltpu.VMEM((8, species), F32)]

    own = call(pack_blocks, [((664, 128), F32)] * 2)(block_inverse, radial_coupling, axial_coupling)
    below = [shift(own[0], "rad_1", 1), None]
    above = [None, shift(own[1], "rad_1", -1)]
    below[1] = shift(own[1], "rad_1", 1)
    above[0] = shift(own[0], "rad_1", -1)
    across = [shift(below[0], "rad_1", 1)]
    across += [shift(above[1], "rad_1", -1)]
    sent = call(
        pack, message, scratch=[pltpu.VMEM((columns, species), F32)], scalars=1
    )(mine, sources)
    got = [sent[0]] + [None] * 3
    for ahead in range(1, GROUP):
        got[GROUP - ahead] = shift(sent[ahead], "rad_1", ahead)
    near_shape = (3, stations, own_cells, species, species)
    taken = call(
        take_near,
        [(near_shape, BF16)] * 2 + [((3, stations, own_cells, 8, species), F32)],
        scratch=rows,
    )(*own, *above, *below)
    high, low, coupling, carry, in_chain = call(
        inner_matrices,
        [square, square, ((stations, cells, 8, species), F32), wide, single],
        scratch=rows,
        scalars=1,
    )(mine, *taken, *across)
    system = (high, low, coupling)
    beside = [(1, 0), (2, 3)]
    in_beside = hop(in_chain, beside)

    source, inner, last = call(first_inner, [field, field, edge], scalars=1)(mine, *got, *system)
    near = hop(last, [(0, 1), (2, 3)])
    out_high, out_low, out_chain = call(outer_matrices, [square, square, single])(*system)
    out_beside = hop(out_chain, beside)
    (joined,) = call(join_plain, [edge])(last, near, in_chain)
    middle = hop(joined, [(1, 2)])
    far = hop(joined, [(1, 3)])
    turn_high, turn_low, turn_chain = call(
        turned_matrices, [square, square, single]
    )(*system, carry)
    outer, ends = call(outer_local, [field, edge])(inner, *system)
    arriving, last = call(turn_first, [edge, edge])(near, middle, far, in_beside, ends, turn_chain)

    for sweep_index in range(SWEEPS):
        if sweep_index:
            count = lax.axis_size("ax")
            up = lax.ppermute(correction, "ax", [(i, i + 1) for i in range(count - 1)])
            down = lax.ppermute(correction, "ax", [(i + 1, i) for i in range(count - 1)])
            inner, last = call(next_inner, [field, edge])(up, correction, down, source, *system)
            near = hop(last, [(0, 1), (1, 0), (2, 3)])
            outer, ends = call(outer_local, [field, edge])(inner, *system)
            (joined,) = call(join, [edge], scalars=1)(places[0], last, near, in_chain, in_beside)
            middle = hop(joined, [(1, 2), (0, 3)])
            arriving, last = call(turn, [edge, edge], scalars=1)(
                places[0], near, middle, in_beside, ends, turn_chain
            )
        near = hop(last, mirrored([(0, 1), (1, 0), (2, 3)]))
        (outer,) = call(deepen, [field])(arriving, outer, turn_high, turn_low)
        (joined,) = call(join, [edge], scalars=1)(places[1], last, near, out_chain, out_beside)
        middle = hop(joined, mirrored([(1, 2), (0, 3)]))
        reach = (near, middle, out_beside, outer, out_high, out_low)
        if sweep_index + 1 < SWEEPS:
            (correction,) = call(finish, [field], scalars=1)(places[1], *reach)
    sent = call(
        finish_last, message, scratch=[pltpu.VMEM(*field)], scalars=2
    )(places[1], mine, *reach)
    got = [sent[0]] + [None] * 3
    for ahead in range(1, GROUP):
        got[GROUP - ahead] = shift(sent[ahead], "rad_1", ahead)
    (correction,) = call(
        unpack, [(sources.shape, F32)], scratch=[pltpu.VMEM((columns, species), F32)], scalars=1
    )(mine, *got)
    return correction


def solution(mesh):
    torus = Mesh(mesh.devices.reshape(mesh.shape["ax"], GROUP, GROUP), ("ax", "rad_0", "rad_1"))
    placed = (P("ax", RAD, None, None),) * 4
    return jax.shard_map(
        relax, mesh=torus, in_specs=placed, out_specs=P("ax", RAD, None, None), check_vma=False
    )
```

```python
import jax
import jax.numpy as jnp
from jax import lax
from jax.experimental import pallas as pl
from jax.experimental.pallas import tpu as pltpu
from jax.sharding import Mesh
from jax.sharding import PartitionSpec as P

SWEEPS = 2
RAD = ("rad_0", "rad_1")
GROUP = 4
F32 = jnp.float32
BF16 = jnp.bfloat16


def split(value):
    high = value.astype(BF16)
    return high, (value - high.astype(F32)).astype(BF16)


def dot(a, b, contract):
    dims = (((1,), (contract,)), ((), ()))
    return lax.dot_general(a, b, dims, preferred_element_type=F32)


def times(value, high, low, contract):
    value_high, value_low = split(value)
    return (
        dot(value_high, high, contract)
        + dot(value_low, high, contract)
        + dot(value_high, low, contract)
    )


def call(body, out, scratch=(), scalars=0):
    def run(*operands):
        specs = [pl.BlockSpec(memory_space=pltpu.SMEM)] * scalars
        specs += [pl.BlockSpec(memory_space=pltpu.VMEM)] * (len(operands) - scalars)
        return pl.pallas_call(
            body,
            out_shape=[jax.ShapeDtypeStruct(shape, kind) for shape, kind in out],
            in_specs=specs,
            out_specs=[pl.BlockSpec(memory_space=pltpu.VMEM)] * len(out),
            scratch_shapes=list(scratch),
            cost_estimate=pl.CostEstimate(
                flops=1000, transcendentals=0, bytes_accessed=1000
            ),
            compiler_params=pltpu.CompilerParams(vmem_limit_bytes=12 * 1024 * 1024),
        )(*operands)

    return run


def pack_blocks(mine_ref, place_ref, block_ref, radial_ref, axial_ref, first, second):
    for station, packed in enumerate((first, second)):
        for cell in range(2):
            packed[200 * cell : 200 * cell + 200] = block_ref[station, cell, :, 0:128]
            packed[400:600, 64 * cell : 64 * cell + 64] = block_ref[station, cell, :, 128:192]
            for chunk in range(7):
                start, stop = 32 * chunk, min(32 * chunk + 32, 200)
                lane = 16 * chunk + 8 * cell
                packed[600 : 600 + stop - start, lane : lane + 8] = block_ref[
                    station, cell, start:stop, 192:200
                ]
            low = 632 + 8 * cell
            packed[low : low + 2] = radial_ref[station, cell, :, 0:128]
            packed[low + 2 : low + 6] = axial_ref[station, cell, :, 0:128]
            packed[low + 16 : low + 18, 0:72] = radial_ref[station, cell, :, 128:200]
            packed[low + 18 : low + 22, 0:72] = axial_ref[station, cell, :, 128:200]


def unpack_block(packed, cell, whole, coupling_whole):
    whole[:, 0:128] = packed[200 * cell : 200 * cell + 200]
    whole[:, 128:192] = packed[400:600, 64 * cell : 64 * cell + 64]
    for chunk in range(7):
        start, stop = 32 * chunk, min(32 * chunk + 32, 200)
        lane = 16 * chunk + 8 * cell
        whole[start:stop, 192:200] = packed[600 : 600 + stop - start, lane : lane + 8]
    low = 632 + 8 * cell
    coupling_whole[:, 0:128] = packed[low : low + 8]
    coupling_whole[:, 128:200] = packed[low + 16 : low + 24, 0:72]
    return split(whole[...]) + (coupling_whole[...],)


def take_near(own0, own1, above0, above1, below0, below1, high, low, coupling, whole, rows):
    for place, pair in enumerate(((own0, own1), (above0, above1), (below0, below1))):
        for station in range(2):
            for cell in range(2):
                block_high, block_low, couple = unpack_block(pair[station], cell, whole, rows)
                high[place, station, cell] = block_high
                low[place, station, cell] = block_low
                coupling[place, station, cell] = couple


def unit_matrix(species):
    rows = lax.broadcasted_iota(jnp.int32, (species, species), 0)
    lanes = lax.broadcasted_iota(jnp.int32, (species, species), 1)
    return jnp.where(rows == lanes, 1.0, 0.0).astype(F32)


def inner_matrices(
    mine_ref, near_high, near_low, near_coupling, across0, across1,
    high, low, coupling, carry, chain, whole, rows,
):
    mine = mine_ref[0]
    for ahead, place in ((0, 0), (1, 1), (3, 2), (2, None)):
        base = lax.rem(mine + ahead, GROUP) * 2
        for station in range(2):
            for cell in range(2):
                if place is None:
                    packed = (across0, across1)[station]
                    parts = unpack_block(packed, cell, whole, rows)
                else:
                    parts = tuple(
                        near[place, station, cell]
                        for near in (near_high, near_low, near_coupling)
                    )
                high[station, base + cell] = parts[0]
                low[station, base + cell] = parts[1]
                coupling[station, base + cell] = parts[2]
    matrix = [unit_matrix(high.shape[2])] * 2
    for cell in range(high.shape[1]):
        for station in range(2):
            inward = coupling[station, cell, 0:1]
            matrix[station] = times(
                -inward * matrix[station], high[station, cell], low[station, cell], 1
            )
            carry[station, cell] = matrix[station]
    for station in range(2):
        chain[station] = matrix[station]


def outer_matrices(high, low, coupling, carry_high, carry_low, chain):
    matrix = [unit_matrix(high.shape[2])] * 2
    for cell in reversed(range(high.shape[1])):
        for station in range(2):
            outward = coupling[station, cell, 1:2]
            matrix[station] = times(
                -outward * matrix[station], high[station, cell], low[station, cell], 1
            )
            part_high, part_low = split(matrix[station])
            carry_high[station, cell] = part_high
            carry_low[station, cell] = part_low
    for station in range(2):
        chain[station] = matrix[station]


def turned_matrices(high, low, coupling, carry, turn_high, turn_low, first):
    matrix = [None, None]
    for cell in reversed(range(high.shape[1])):
        for station in range(2):
            whole = carry[station, cell]
            if matrix[station] is not None:
                outward = coupling[station, cell, 1:2]
                whole = whole - times(
                    outward * matrix[station], high[station, cell], low[station, cell], 1
                )
            matrix[station] = whole
            part_high, part_low = split(whole)
            turn_high[station, cell] = part_high
            turn_low[station, cell] = part_low
    for station in range(2):
        first[station] = matrix[station]


def pack(mine_ref, sources_ref, m0, m1, m2, m3, turned):
    mine = mine_ref[0]
    width = m0.shape[2]
    for station in range(2):
        for cell in range(2):
            turned[...] = sources_ref[station, cell].T
            for ahead, message in enumerate((m0, m1, m2, m3)):
                row = pl.multiple_of(lax.rem(mine + ahead, GROUP) * width, 8)
                message[station, cell] = turned[pl.ds(row, width)]


def first_inner(mine_ref, m0, m1, m2, m3, high, low, coupling, sources, local, last):
    mine = mine_ref[0]
    for station in range(2):
        for ahead, message in enumerate((m0, m1, m2, m3)):
            base = lax.rem(mine + ahead, GROUP) * 2
            for cell in range(2):
                sources[station, base + cell] = message[station, cell]
    inner_chain(lambda station, cell: sources[station, cell], high, low, coupling, local, last)


def inner_chain(source_of, high, low, coupling, local, last):
    value = [None, None]
    for cell in range(high.shape[1]):
        for station in range(2):
            shifted = source_of(station, cell)
            if value[station] is not None:
                shifted = shifted - coupling[station, cell, 0:1] * value[station]
            value[station] = times(shifted, high[station, cell], low[station, cell], 1)
            local[station, cell] = value[station]
    for station in range(2):
        last[station] = value[station]


def next_inner(below, own, above, sources, high, low, coupling, local, last):
    def source_of(station, cell):
        around = [part[s, cell] for part in (below, own, above) for s in range(2)]
        source = sources[station, cell]
        for term, place in enumerate((0, 1, 3, 4)):
            source = source - coupling[station, cell, 2 + term : 3 + term] * around[station + place]
        return source

    inner_chain(source_of, high, low, coupling, local, last)


def outer_local(inner, high, low, coupling, local, last):
    value = [None, None]
    for cell in reversed(range(high.shape[1])):
        for station in range(2):
            whole = inner[station, cell]
            if value[station] is not None:
                shifted = coupling[station, cell, 1:2] * value[station]
                whole = whole - times(shifted, high[station, cell], low[station, cell], 1)
            value[station] = whole
            local[station, cell] = whole
    for station in range(2):
        last[station] = value[station]


def by_matrix(value, matrix):
    high, low = split(matrix)
    return times(value, high, low, 0)


def join_plain(ends, near, chain, joined):
    for station in range(2):
        joined[station] = ends[station] + by_matrix(near[station], chain[station])


def join(outermost, ends, near, chain, chain_beside, joined):
    for station in range(2):
        mine, other = ends[station], near[station]
        matrix = jnp.where(outermost, chain_beside[station], chain[station])
        joined[station] = jnp.where(outermost, other, mine) + by_matrix(
            jnp.where(outermost, mine, other), matrix
        )


def join_inner(place_ref, *refs):
    join(place_ref[0] == 0, *refs)


def join_outer(place_ref, *refs):
    join(place_ref[0] == GROUP - 1, *refs)


def incoming(place, near, middle, chain_beside, station):
    far = by_matrix(middle[station], chain_beside[station])
    arriving = near[station] + jnp.where(place == GROUP - 1, far, middle[station])
    return jnp.where(place == 0, 0.0, arriving)


def turn_first(near, middle, far, chain_beside, ends, matrix, arriving, turned):
    for station in range(2):
        value = near[station] + middle[station] + by_matrix(far[station], chain_beside[station])
        arriving[station] = value
        turned[station] = ends[station] + by_matrix(value, matrix[station])


def turn(place_ref, near, middle, chain_beside, ends, matrix, arriving, turned):
    for station in range(2):
        value = incoming(place_ref[0], near, middle, chain_beside, station)
        arriving[station] = value
        turned[station] = ends[station] + by_matrix(value, matrix[station])


def deepen(arriving, outer, turn_high, turn_low, deeper):
    for station in range(2):
        value = arriving[station]
        for cell in range(outer.shape[1]):
            deeper[station, cell] = outer[station, cell] + times(
                value, turn_high[station, cell], turn_low[station, cell], 0
            )


def finish(place_ref, near, middle, chain_beside, outer, carry_high, carry_low, correction):
    place = GROUP - 1 - place_ref[0]
    for station in range(2):
        arriving = incoming(place, near, middle, chain_beside, station)
        for cell in range(outer.shape[1]):
            correction[station, cell] = outer[station, cell] + times(
                arriving, carry_high[station, cell], carry_low[station, cell], 0
            )


def finish_last(
    place_ref, mine_ref, near, middle, chain_beside, outer, carry_high, carry_low,
    m0, m1, m2, m3, whole,
):
    finish(place_ref, near, middle, chain_beside, outer, carry_high, carry_low, whole)
    mine = mine_ref[0]
    for station in range(2):
        for ahead, message in enumerate((m0, m1, m2, m3)):
            base = lax.rem(mine + ahead, GROUP) * 2
            for cell in range(2):
                message[station, cell] = whole[station, base + cell]


def unpack(mine_ref, m0, m1, m2, m3, correction, turned):
    mine = mine_ref[0]
    width = m0.shape[2]
    for station in range(2):
        for cell in range(2):
            for ahead, message in enumerate((m0, m1, m2, m3)):
                row = pl.multiple_of(lax.rem(mine + ahead, GROUP) * width, 8)
                turned[pl.ds(row, width)] = message[station, cell]
            correction[station, cell] = turned[...].T


def shift(value, axis, step):
    count = lax.axis_size(axis)
    return lax.ppermute(value, axis, [(i, (i + step) % count) for i in range(count)])


def hop(value, pairs):
    return lax.ppermute(value, "rad_0", pairs)


def mirrored(pairs):
    return [(GROUP - 1 - source, GROUP - 1 - target) for source, target in pairs]


def relax(sources, block_inverse, radial_coupling, axial_coupling):
    stations, own_cells, species, columns = sources.shape
    cells = own_cells * GROUP
    width = columns // GROUP
    mine = lax.axis_index("rad_1").astype(jnp.int32).reshape(1)
    place = lax.axis_index("rad_0").astype(jnp.int32).reshape(1)
    field = ((stations, cells, width, species), F32)
    square = ((stations, cells, species, species), BF16)
    wide = ((stations, cells, species, species), F32)
    edge = ((stations, width, species), F32)
    single = ((stations, species, species), F32)
    message = [((stations, own_cells, width, species), F32)] * GROUP
    rows = [pltpu.VMEM((species, species), F32), pltpu.VMEM((8, species), F32)]

    own = call(pack_blocks, [((664, 128), F32)] * 2, scalars=2)(
        mine, place, block_inverse, radial_coupling, axial_coupling
    )
    below = [shift(own[0], "rad_1", 1), None]
    above = [None, shift(own[1], "rad_1", -1)]
    below[1] = shift(own[1], "rad_1", 1)
    above[0] = shift(own[0], "rad_1", -1)
    across = [shift(below[0], "rad_1", 1)]
    across += [shift(above[1], "rad_1", -1)]
    sent = call(
        pack, message, scratch=[pltpu.VMEM((columns, species), F32)], scalars=1
    )(mine, sources)
    got = [sent[0]] + [None] * 3
    for ahead in range(1, GROUP):
        got[GROUP - ahead] = shift(sent[ahead], "rad_1", ahead)
    near_shape = (3, stations, own_cells, species, species)
    taken = call(
        take_near,
        [(near_shape, BF16)] * 2 + [((3, stations, own_cells, 8, species), F32)],
        scratch=rows,
    )(*own, *above, *below)
    high, low, coupling, carry, in_chain = call(
        inner_matrices,
        [square, square, ((stations, cells, 8, species), F32), wide, single],
        scratch=rows,
        scalars=1,
    )(mine, *taken, *across)
    system = (high, low, coupling)
    beside = [(1, 0), (2, 3)]
    in_beside = hop(in_chain, beside)

    source, inner, last = call(first_inner, [field, field, edge], scalars=1)(mine, *got, *system)
    near = hop(last, [(0, 1), (2, 3)])
    out_high, out_low, out_chain = call(outer_matrices, [square, square, single])(*system)
    out_beside = hop(out_chain, beside)
    (joined,) = call(join_plain, [edge])(last, near, in_chain)
    middle = hop(joined, [(1, 2)])
    far = hop(joined, [(1, 3)])
    turn_high, turn_low, turn_chain = call(
        turned_matrices, [square, square, single]
    )(*system, carry)
    outer, ends = call(outer_local, [field, edge])(inner, *system)
    arriving, last = call(turn_first, [edge, edge])(near, middle, far, in_beside, ends, turn_chain)

    for sweep_index in range(SWEEPS):
        if sweep_index:
            count = lax.axis_size("ax")
            up = lax.ppermute(correction, "ax", [(i, i + 1) for i in range(count - 1)])
            down = lax.ppermute(correction, "ax", [(i + 1, i) for i in range(count - 1)])
            inner, last = call(next_inner, [field, edge])(up, correction, down, source, *system)
            near = hop(last, [(0, 1), (1, 0), (2, 3)])
            outer, ends = call(outer_local, [field, edge])(inner, *system)
            (joined,) = call(join_inner, [edge], scalars=1)(place, last, near, in_chain, in_beside)
            middle = hop(joined, [(1, 2), (0, 3)])
            arriving, last = call(turn, [edge, edge], scalars=1)(
                place, near, middle, in_beside, ends, turn_chain
            )
        near = hop(last, mirrored([(0, 1), (1, 0), (2, 3)]))
        (outer,) = call(deepen, [field])(arriving, outer, turn_high, turn_low)
        (joined,) = call(join_outer, [edge], scalars=1)(place, last, near, out_chain, out_beside)
        middle = hop(joined, mirrored([(1, 2), (0, 3)]))
        reach = (near, middle, out_beside, outer, out_high, out_low)
        if sweep_index + 1 < SWEEPS:
            (correction,) = call(finish, [field], scalars=1)(place, *reach)
    sent = call(finish_last, message, scratch=[pltpu.VMEM(*field)], scalars=2)(place, mine, *reach)
    got = [sent[0]] + [None] * 3
    for ahead in range(1, GROUP):
        got[GROUP - ahead] = shift(sent[ahead], "rad_1", ahead)
    (correction,) = call(
        unpack, [(sources.shape, F32)], scratch=[pltpu.VMEM((columns, species), F32)], scalars=1
    )(mine, *got)
    return correction


def solution(mesh):
    torus = Mesh(mesh.devices.reshape(mesh.shape["ax"], GROUP, GROUP), ("ax", "rad_0", "rad_1"))
    placed = (P("ax", RAD, None, None),) * 4
    return jax.shard_map(
        relax, mesh=torus, in_specs=placed, out_specs=P("ax", RAD, None, None), check_vma=False
    )
```

```python
import jax
import jax.numpy as jnp
from jax import lax
from jax.experimental import pallas as pl
from jax.experimental.pallas import tpu as pltpu
from jax.sharding import Mesh
from jax.sharding import PartitionSpec as P

SWEEPS = 2
RAD = ("rad_0", "rad_1")
GROUP = 4
F32 = jnp.float32
BF16 = jnp.bfloat16


def split(value):
    high = value.astype(BF16)
    return high, (value - high.astype(F32)).astype(BF16)


def dot(a, b, contract):
    dims = (((1,), (contract,)), ((), ()))
    return lax.dot_general(a, b, dims, preferred_element_type=F32)


def times(value, high, low, contract):
    value_high, value_low = split(value)
    return (
        dot(value_high, high, contract)
        + dot(value_low, high, contract)
        + dot(value_high, low, contract)
    )


def call(body, out, scratch=(), scalars=0, space=pltpu.VMEM):
    def run(*operands):
        specs = [pl.BlockSpec(memory_space=pltpu.SMEM)] * scalars
        specs += [pl.BlockSpec(memory_space=space)] * (len(operands) - scalars)
        moved = sum(o.size * o.dtype.itemsize for o in operands)
        return pl.pallas_call(
            body,
            out_shape=[jax.ShapeDtypeStruct(shape, kind) for shape, kind in out],
            in_specs=specs,
            out_specs=[pl.BlockSpec(memory_space=pltpu.VMEM)] * len(out),
            scratch_shapes=list(scratch),
            cost_estimate=pl.CostEstimate(
                flops=1000, transcendentals=0, bytes_accessed=1000
            ),
            compiler_params=pltpu.CompilerParams(vmem_limit_bytes=12 * 1024 * 1024),
        )(*operands)

    return run


def pack_blocks(
    mine_ref, place_ref, block_far, radial_far, axial_far, first, second,
    block_ref, radial_ref, axial_ref, arrives,
):
    pairs = [(block_far.at[s], block_ref.at[s]) for s in range(2)]
    pairs += [(radial_far, radial_ref), (axial_far, axial_ref)]
    copies = [
        pltpu.make_async_copy(source, target, arrives.at[k])
        for k, (source, target) in enumerate(pairs)
    ]
    for copy in copies:
        copy.start()
    for station, packed in enumerate((first, second)):
        copies[station].wait()
        if not station:
            copies[2].wait()
            copies[3].wait()
        for cell in range(2):
            packed[200 * cell : 200 * cell + 200] = block_ref[station, cell, :, 0:128]
            packed[400:600, 64 * cell : 64 * cell + 64] = block_ref[station, cell, :, 128:192]
            for chunk in range(7):
                start, stop = 32 * chunk, min(32 * chunk + 32, 200)
                lane = 16 * chunk + 8 * cell
                packed[600 : 600 + stop - start, lane : lane + 8] = block_ref[
                    station, cell, start:stop, 192:200
                ]
            low = 632 + 8 * cell
            packed[low : low + 2] = radial_ref[station, cell, :, 0:128]
            packed[low + 2 : low + 6] = axial_ref[station, cell, :, 0:128]
            packed[low + 16 : low + 18, 0:72] = radial_ref[station, cell, :, 128:200]
            packed[low + 18 : low + 22, 0:72] = axial_ref[station, cell, :, 128:200]


def unpack_block(packed, cell, whole, coupling_whole):
    whole[:, 0:128] = packed[200 * cell : 200 * cell + 200]
    whole[:, 128:192] = packed[400:600, 64 * cell : 64 * cell + 64]
    for chunk in range(7):
        start, stop = 32 * chunk, min(32 * chunk + 32, 200)
        lane = 16 * chunk + 8 * cell
        whole[start:stop, 192:200] = packed[600 : 600 + stop - start, lane : lane + 8]
    low = 632 + 8 * cell
    coupling_whole[:, 0:128] = packed[low : low + 8]
    coupling_whole[:, 128:200] = packed[low + 16 : low + 24, 0:72]
    return split(whole[...]) + (coupling_whole[...],)


def take_near(own0, own1, above0, above1, below0, below1, high, low, coupling, whole, rows):
    for place, pair in enumerate(((own0, own1), (above0, above1), (below0, below1))):
        for station in range(2):
            for cell in range(2):
                block_high, block_low, couple = unpack_block(pair[station], cell, whole, rows)
                high[place, station, cell] = block_high
                low[place, station, cell] = block_low
                coupling[place, station, cell] = couple


def unit_matrix(species):
    rows = lax.broadcasted_iota(jnp.int32, (species, species), 0)
    lanes = lax.broadcasted_iota(jnp.int32, (species, species), 1)
    return jnp.where(rows == lanes, 1.0, 0.0).astype(F32)


def inner_matrices(
    mine_ref, near_high, near_low, near_coupling, across0, across1,
    high, low, coupling, carry, chain, whole, rows,
):
    mine = mine_ref[0]
    for ahead, place in ((0, 0), (1, 1), (3, 2), (2, None)):
        base = lax.rem(mine + ahead, GROUP) * 2
        for station in range(2):
            for cell in range(2):
                if place is None:
                    packed = (across0, across1)[station]
                    parts = unpack_block(packed, cell, whole, rows)
                else:
                    parts = tuple(
                        near[place, station, cell]
                        for near in (near_high, near_low, near_coupling)
                    )
                high[station, base + cell] = parts[0]
                low[station, base + cell] = parts[1]
                coupling[station, base + cell] = parts[2]
    matrix = [unit_matrix(high.shape[2])] * 2
    for cell in range(high.shape[1]):
        for station in range(2):
            inward = coupling[station, cell, 0:1]
            matrix[station] = times(
                -inward * matrix[station], high[station, cell], low[station, cell], 1
            )
            carry[station, cell] = matrix[station]
    for station in range(2):
        chain[station] = matrix[station]


def outer_matrices(high, low, coupling, carry_high, carry_low, chain):
    matrix = [unit_matrix(high.shape[2])] * 2
    for cell in reversed(range(high.shape[1])):
        for station in range(2):
            outward = coupling[station, cell, 1:2]
            matrix[station] = times(
                -outward * matrix[station], high[station, cell], low[station, cell], 1
            )
            part_high, part_low = split(matrix[station])
            carry_high[station, cell] = part_high
            carry_low[station, cell] = part_low
    for station in range(2):
        chain[station] = matrix[station]


def turned_matrices(high, low, coupling, carry, turn_high, turn_low, first):
    matrix = [None, None]
    for cell in reversed(range(high.shape[1])):
        for station in range(2):
            whole = carry[station, cell]
            if matrix[station] is not None:
                outward = coupling[station, cell, 1:2]
                whole = whole - times(
                    outward * matrix[station], high[station, cell], low[station, cell], 1
                )
            matrix[station] = whole
            part_high, part_low = split(whole)
            turn_high[station, cell] = part_high
            turn_low[station, cell] = part_low
    for station in range(2):
        first[station] = matrix[station]


def pack(mine_ref, sources_ref, m0, m1, m2, m3, turned):
    mine = mine_ref[0]
    width = m0.shape[2]
    for station in range(2):
        for cell in range(2):
            turned[...] = sources_ref[station, cell].T
            for ahead, message in enumerate((m0, m1, m2, m3)):
                row = pl.multiple_of(lax.rem(mine + ahead, GROUP) * width, 8)
                message[station, cell] = turned[pl.ds(row, width)]


def first_inner(mine_ref, m0, m1, m2, m3, high, low, coupling, sources, local, last):
    mine = mine_ref[0]
    for station in range(2):
        for ahead, message in enumerate((m0, m1, m2, m3)):
            base = lax.rem(mine + ahead, GROUP) * 2
            for cell in range(2):
                sources[station, base + cell] = message[station, cell]
    inner_chain(lambda station, cell: sources[station, cell], high, low, coupling, local, last)


def inner_chain(source_of, high, low, coupling, local, last):
    value = [None, None]
    for cell in range(high.shape[1]):
        for station in range(2):
            shifted = source_of(station, cell)
            if value[station] is not None:
                shifted = shifted - coupling[station, cell, 0:1] * value[station]
            value[station] = times(shifted, high[station, cell], low[station, cell], 1)
            local[station, cell] = value[station]
    for station in range(2):
        last[station] = value[station]


def next_inner(below, own, above, sources, high, low, coupling, local, last):
    def source_of(station, cell):
        around = [part[s, cell] for part in (below, own, above) for s in range(2)]
        source = sources[station, cell]
        for term, place in enumerate((0, 1, 3, 4)):
            source = source - coupling[station, cell, 2 + term : 3 + term] * around[station + place]
        return source

    inner_chain(source_of, high, low, coupling, local, last)


def outer_local(inner, high, low, coupling, local, last):
    value = [None, None]
    for cell in reversed(range(high.shape[1])):
        for station in range(2):
            whole = inner[station, cell]
            if value[station] is not None:
                shifted = coupling[station, cell, 1:2] * value[station]
                whole = whole - times(shifted, high[station, cell], low[station, cell], 1)
            value[station] = whole
            local[station, cell] = whole
    for station in range(2):
        last[station] = value[station]


def by_matrix(value, matrix):
    high, low = split(matrix)
    return times(value, high, low, 0)


def join_plain(ends, near, chain, joined):
    for station in range(2):
        joined[station] = ends[station] + by_matrix(near[station], chain[station])


def join(outermost, ends, near, chain, chain_beside, joined):
    for station in range(2):
        mine, other = ends[station], near[station]
        matrix = jnp.where(outermost, chain_beside[station], chain[station])
        joined[station] = jnp.where(outermost, other, mine) + by_matrix(
            jnp.where(outermost, mine, other), matrix
        )


def join_inner(place_ref, *refs):
    join(place_ref[0] == 0, *refs)


def join_outer(place_ref, *refs):
    join(place_ref[0] == GROUP - 1, *refs)


def incoming(place, near, middle, chain_beside, station):
    far = by_matrix(middle[station], chain_beside[station])
    arriving = near[station] + jnp.where(place == GROUP - 1, far, middle[station])
    return jnp.where(place == 0, 0.0, arriving)


def turn_first(near, middle, far, chain_beside, ends, matrix, arriving, turned):
    for station in range(2):
        value = near[station] + middle[station] + by_matrix(far[station], chain_beside[station])
        arriving[station] = value
        turned[station] = ends[station] + by_matrix(value, matrix[station])


def turn(place_ref, near, middle, chain_beside, ends, matrix, arriving, turned):
    for station in range(2):
        value = incoming(place_ref[0], near, middle, chain_beside, station)
        arriving[station] = value
        turned[station] = ends[station] + by_matrix(value, matrix[station])


def deepen(arriving, outer, turn_high, turn_low, deeper):
    for station in range(2):
        value = arriving[station]
        for cell in range(outer.shape[1]):
            deeper[station, cell] = outer[station, cell] + times(
                value, turn_high[station, cell], turn_low[station, cell], 0
            )


def finish(place_ref, near, middle, chain_beside, outer, carry_high, carry_low, correction):
    place = GROUP - 1 - place_ref[0]
    for station in range(2):
        arriving = incoming(place, near, middle, chain_beside, station)
        for cell in range(outer.shape[1]):
            correction[station, cell] = outer[station, cell] + times(
                arriving, carry_high[station, cell], carry_low[station, cell], 0
            )


def finish_last(
    place_ref, mine_ref, near, middle, chain_beside, outer, carry_high, carry_low,
    m0, m1, m2, m3, whole,
):
    finish(place_ref, near, middle, chain_beside, outer, carry_high, carry_low, whole)
    mine = mine_ref[0]
    for station in range(2):
        for ahead, message in enumerate((m0, m1, m2, m3)):
            base = lax.rem(mine + ahead, GROUP) * 2
            for cell in range(2):
                message[station, cell] = whole[station, base + cell]


def unpack(mine_ref, m0, m1, m2, m3, correction, turned):
    mine = mine_ref[0]
    width = m0.shape[2]
    for station in range(2):
        for cell in range(2):
            for ahead, message in enumerate((m0, m1, m2, m3)):
                row = pl.multiple_of(lax.rem(mine + ahead, GROUP) * width, 8)
                turned[pl.ds(row, width)] = message[station, cell]
            correction[station, cell] = turned[...].T


def shift(value, axis, step):
    count = lax.axis_size(axis)
    return lax.ppermute(value, axis, [(i, (i + step) % count) for i in range(count)])


def hop(value, pairs):
    return lax.ppermute(value, "rad_0", pairs)


def mirrored(pairs):
    return [(GROUP - 1 - source, GROUP - 1 - target) for source, target in pairs]


def relax(sources, block_inverse, radial_coupling, axial_coupling):
    stations, own_cells, species, columns = sources.shape
    cells = own_cells * GROUP
    width = columns // GROUP
    mine = lax.axis_index("rad_1").astype(jnp.int32).reshape(1)
    place = lax.axis_index("rad_0").astype(jnp.int32).reshape(1)
    field = ((stations, cells, width, species), F32)
    square = ((stations, cells, species, species), BF16)
    wide = ((stations, cells, species, species), F32)
    edge = ((stations, width, species), F32)
    single = ((stations, species, species), F32)
    message = [((stations, own_cells, width, species), F32)] * GROUP
    rows = [pltpu.VMEM((species, species), F32), pltpu.VMEM((8, species), F32)]

    arrays = (block_inverse, radial_coupling, axial_coupling)
    own = call(
        pack_blocks,
        [((664, 128), F32)] * 2,
        scratch=[pltpu.VMEM(array.shape, F32) for array in arrays]
        + [pltpu.SemaphoreType.DMA((4,))],
        scalars=2,
        space=pltpu.HBM,
    )(mine, place, *(pltpu.with_memory_space_constraint(array, pltpu.HBM) for array in arrays))
    below = [shift(own[0], "rad_1", 1), None]
    above = [None, shift(own[1], "rad_1", -1)]
    below[1] = shift(own[1], "rad_1", 1)
    above[0] = shift(own[0], "rad_1", -1)
    across = [shift(below[0], "rad_1", 1)]
    across += [shift(above[1], "rad_1", -1)]
    sent = call(
        pack, message, scratch=[pltpu.VMEM((columns, species), F32)], scalars=1
    )(mine, sources)
    got = [sent[0]] + [None] * 3
    for ahead in range(1, GROUP):
        got[GROUP - ahead] = shift(sent[ahead], "rad_1", ahead)
    near_shape = (3, stations, own_cells, species, species)
    taken = call(
        take_near,
        [(near_shape, BF16)] * 2 + [((3, stations, own_cells, 8, species), F32)],
        scratch=rows,
    )(*own, *above, *below)
    high, low, coupling, carry, in_chain = call(
        inner_matrices,
        [square, square, ((stations, cells, 8, species), F32), wide, single],
        scratch=rows,
        scalars=1,
    )(mine, *taken, *across)
    system = (high, low, coupling)
    beside = [(1, 0), (2, 3)]
    in_beside = hop(in_chain, beside)

    source, inner, last = call(first_inner, [field, field, edge], scalars=1)(mine, *got, *system)
    near = hop(last, [(0, 1), (2, 3)])
    out_high, out_low, out_chain = call(outer_matrices, [square, square, single])(*system)
    out_beside = hop(out_chain, beside)
    (joined,) = call(join_plain, [edge])(last, near, in_chain)
    middle = hop(joined, [(1, 2)])
    far = hop(joined, [(1, 3)])
    turn_high, turn_low, turn_chain = call(
        turned_matrices, [square, square, single]
    )(*system, carry)
    outer, ends = call(outer_local, [field, edge])(inner, *system)
    arriving, last = call(turn_first, [edge, edge])(near, middle, far, in_beside, ends, turn_chain)

    for sweep_index in range(SWEEPS):
        if sweep_index:
            count = lax.axis_size("ax")
            up = lax.ppermute(correction, "ax", [(i, i + 1) for i in range(count - 1)])
            down = lax.ppermute(correction, "ax", [(i + 1, i) for i in range(count - 1)])
            inner, last = call(next_inner, [field, edge])(up, correction, down, source, *system)
            near = hop(last, [(0, 1), (1, 0), (2, 3)])
            outer, ends = call(outer_local, [field, edge])(inner, *system)
            (joined,) = call(join_inner, [edge], scalars=1)(place, last, near, in_chain, in_beside)
            middle = hop(joined, [(1, 2), (0, 3)])
            arriving, last = call(turn, [edge, edge], scalars=1)(
                place, near, middle, in_beside, ends, turn_chain
            )
        near = hop(last, mirrored([(0, 1), (1, 0), (2, 3)]))
        (outer,) = call(deepen, [field])(arriving, outer, turn_high, turn_low)
        (joined,) = call(join_outer, [edge], scalars=1)(place, last, near, out_chain, out_beside)
        middle = hop(joined, mirrored([(1, 2), (0, 3)]))
        reach = (near, middle, out_beside, outer, out_high, out_low)
        if sweep_index + 1 < SWEEPS:
            (correction,) = call(finish, [field], scalars=1)(place, *reach)
    sent = call(finish_last, message, scratch=[pltpu.VMEM(*field)], scalars=2)(place, mine, *reach)
    got = [sent[0]] + [None] * 3
    for ahead in range(1, GROUP):
        got[GROUP - ahead] = shift(sent[ahead], "rad_1", ahead)
    (correction,) = call(
        unpack, [(sources.shape, F32)], scratch=[pltpu.VMEM((columns, species), F32)], scalars=1
    )(mine, *got)
    return correction


def solution(mesh):
    torus = Mesh(mesh.devices.reshape(mesh.shape["ax"], GROUP, GROUP), ("ax", "rad_0", "rad_1"))
    placed = (P("ax", RAD, None, None),) * 4
    return jax.shard_map(
        relax, mesh=torus, in_specs=placed, out_specs=P("ax", RAD, None, None), check_vma=False
    )
```
